16 devices in a mesh: rep: 1, r: 2 (over z), s: 8 (over x, y, core).
Axes of the slice: x: 2, y: 2, z: 2, core: 2. Of those that a mesh axis runs over, the one named last changes fastest.
Arguments:
- x: bfloat16 [16, 2048, 1280], P(('rep', 'r', 's'))
- dy: bfloat16 [16, 2048, 1280], P(('rep', 'r', 's'))
- w_gate: bfloat16 [2, 1280, 3072], P(None, 's')
- w_up: bfloat16 [2, 1280, 3072], P(None, 's')
- w_down: bfloat16 [2, 3072, 1280], P(None, 's')
Outputs:
- output 1: bfloat16 [16, 2048, 1280], P(('rep', 'r', 's'))
- output 2: bfloat16 [2, 1280, 3072], P('rep', 's')
- output 3: bfloat16 [2, 1280, 3072], P('rep', 's')
- output 4: bfloat16 [2, 3072, 1280], P('rep', 's')
All inputs are finite; a program needn't handle non-finite values.
Results may differ from the reference program's by a relative error of at most 0.018.
Values are sent between devices in bfloat16 or wider.
A program may use at most 2 GiB of HBM per device.

```python
import jax
import jax.numpy as jnp
from jax import lax

SEQUENCES = 16
TOKENS = 2048
D = 1280
FF = 3072
LAYERS = 2
NAMES = ("w_gate", "w_up", "w_down")
SHAPES = {"w_gate": (LAYERS, D, FF), "w_up": (LAYERS, D, FF), "w_down": (LAYERS, FF, D)}


def bump(key, n, height):
    away = (jnp.arange(n, dtype=jnp.int32) - jax.random.randint(key, (), 0, n, jnp.int32)) % n
    return jnp.where(away < n // 8, height, 1.0)


def together(key, own, strength):
    shared = jax.random.normal(key, own.shape[1:], jnp.float32)
    return (own + strength * shared) * lax.rsqrt(1 + strength * strength)


def setup_inputs(seed: int = 0, part: int = 0) -> dict:
    kx, kdy, ka, kb, kz, kf, kh, kl, *kw = jax.random.split(jax.random.key(seed), 8 + len(NAMES))
    kx, kdy, ka, kb = (jax.random.fold_in(k, part) for k in (kx, kdy, ka, kb))
    shape = (SEQUENCES, TOKENS, D)
    much_x, much_dy = jax.random.uniform(kz, (2,), jnp.float32, 0.0, 1.0)
    layers = 2.0 ** jax.random.uniform(kl, (LAYERS, 1, 1), jnp.float32, -1.0, 1.0)
    x = together(ka, jax.random.normal(kx, shape, jnp.float32), much_x) * bump(kf, D, 4.0)
    dy = together(kb, jax.random.normal(kdy, shape, jnp.float32), much_dy)
    drawn = {"x": x.astype(jnp.bfloat16), "dy": (dy * (SEQUENCES * TOKENS) ** -0.5).astype(jnp.bfloat16)}
    for key, name in zip(kw, NAMES, strict=True):
        w = jax.random.normal(key, SHAPES[name], jnp.float32) * SHAPES[name][1] ** -0.5
        drawn[name] = (w * {"w_gate": 1.0, "w_up": bump(kh, FF, 4.0), "w_down": layers}[name]).astype(jnp.bfloat16)
    return drawn


def matmul(a, w):
    return jnp.dot(a, w, preferred_element_type=jnp.float32).astype(jnp.bfloat16)


def normed(h):
    wide = h.astype(jnp.float32)
    scale = lax.rsqrt(jnp.mean(wide**2, -1, keepdims=True) + 1e-6)
    return (wide * scale).astype(jnp.bfloat16)


def layer(h, w):
    a = normed(h)
    gate = jnp.dot(a, w["w_gate"], preferred_element_type=jnp.float32)
    up = jnp.dot(a, w["w_up"], preferred_element_type=jnp.float32)
    return h + matmul((jax.nn.silu(gate) * up).astype(jnp.bfloat16), w["w_down"])


def stack(weights, h):
    return lax.scan(lambda h, w: (layer(h, w), None), h, weights)[0]


def reference(x, dy, w_gate, w_up, w_down):
    weights = dict(zip(NAMES, (w_gate, w_up, w_down), strict=True))

    def take(so_far, sequence):
        h, by_y = sequence
        _, back = jax.vjp(stack, weights, h)
        by_weights, by_h = back(by_y)
        return jax.tree.map(lambda total, term: total + term.astype(jnp.float32), so_far, by_weights), by_h

    none_yet = {name: jnp.zeros(w.shape, jnp.float32) for name, w in weights.items()}
    by_weights, by_x = lax.scan(take, none_yet, (x, dy))
    return (by_x, *(by_weights[name].astype(jnp.bfloat16) for name in NAMES))
```

```python
import functools

import jax
import jax.numpy as jnp
from jax import lax
from jax.experimental import pallas as pl
from jax.experimental.pallas import tpu as pltpu
from jax.sharding import PartitionSpec as P

MESH = pl.DeviceIdType.MESH
BF, F32 = jnp.bfloat16, jnp.float32
ANY = pl.BlockSpec(memory_space=pl.ANY)
VMEM_LIMIT = 66_000_000
TOK, D, FF = 2048, 1280, 3072


class Place:
    def __init__(self):
        self.z = lax.axis_index("r")
        self.s = lax.axis_index("s")
        self.x = self.s // 4
        self.y = (self.s // 2) % 2
        self.c = self.s % 2
        self.xs = self.s + 4 - 8 * self.x
        self.ys = self.s + 2 - 4 * self.y
        self.sib = self.s + 1 - 2 * self.c
        self.ds = self.xs + 2 - 4 * self.y
        self.to_x, self.to_y, self.to_sib = {"s": self.xs}, {"s": self.ys}, {"s": self.sib}
        self.to_z = {"r": 1 - self.z}

    def greet(self):
        barrier = pltpu.get_barrier_semaphore()
        for peer in (self.to_x, self.to_y, self.to_sib, self.to_z):
            pl.semaphore_signal(barrier, inc=1, device_id=peer, device_id_type=MESH)
        pl.semaphore_wait(barrier, 4)


def remote(src, dst, sems, k, peer):
    return pltpu.make_async_remote_copy(
        src_ref=src, dst_ref=dst, send_sem=sems[0].at[k], recv_sem=sems[1].at[k], device_id=peer, device_id_type=MESH
    )


class Gather:
    copies = 14
    stages = 4

    def __init__(self, own):
        self.inputs = [own]
        self.outputs = [jax.ShapeDtypeStruct((8, *own.shape), own.dtype)]
        self.scratch = [
            pltpu.VMEM(own.shape, own.dtype),
            pltpu.SemaphoreType.DMA((2,)),
            pltpu.SemaphoreType.DMA((self.copies,)),
            pltpu.SemaphoreType.DMA((self.copies,)),
        ]

    def stage(self, at, number, ins, outs, scratch):
        (own,), (full,), (held, local, *sems) = ins, outs, scratch
        rows = own.shape[0]
        low = 48 if rows == 160 else rows // 3
        both = rows - low
        plane = pl.ds(pl.multiple_of(at.z * low, 16), both)
        middle = pl.ds(low, both - low)
        mine = pl.ds(pl.multiple_of(at.z * both, 16), low)
        theirs = pl.ds(pl.multiple_of((1 - at.z) * both, 16), low)

        def copy(k):
            block = lambda s, r: full.at[s, r, :]
            return {
                0: lambda: remote(own.at[plane, :], block(at.s, plane), sems, 0, at.to_x),
                1: lambda: remote(own.at[plane, :], block(at.s, plane), sems, 1, at.to_y),
                2: lambda: remote(own, full.at[at.s], sems, 2, at.to_sib),
                3: lambda: remote(block(at.xs, middle), block(at.xs, middle), sems, 3, at.to_y),
                4: lambda: remote(block(at.ys, mine), block(at.ys, mine), sems, 4, at.to_x),
                5: lambda: remote(block(at.xs, mine), block(at.xs, mine), sems, 5, at.to_z),
                6: lambda: remote(block(at.ys, mine), block(at.ys, mine), sems, 6, at.to_z),
                7: lambda: remote(block(at.xs, plane), block(at.xs, plane), sems, 7, at.to_sib),
                8: lambda: remote(block(at.ys, plane), block(at.ys, plane), sems, 8, at.to_sib),
                9: lambda: remote(block(at.ds, mine), block(at.ds, mine), sems, 9, at.to_z),
                10: lambda: remote(block(at.ds, plane), block(at.ds, plane), sems, 10, at.to_sib),
                11: lambda: remote(block(at.xs, theirs), block(at.xs, theirs), sems, 11, at.to_sib),
                12: lambda: remote(block(at.ys, theirs), block(at.ys, theirs), sems, 12, at.to_sib),
                13: lambda: remote(block(at.ds, theirs), block(at.ds, theirs), sems, 13, at.to_sib),
            }[k]()

        into = lambda: pltpu.make_async_copy(own, held, local.at[0])
        out = lambda: pltpu.make_async_copy(held, full.at[at.s], local.at[1])
        wait, start = {
            0: ((), (0, 1, 2)),
            1: ((0, 1), (3, 4, 5, 6, 7, 8)),
            2: ((3, 4), (9, 10)),
            3: ((5, 6, 9), (11, 12, 13)),
            4: ((2, 7, 8, 10, 11, 12, 13), ()),
        }[number]
        if number == 1:
            into().wait()
            out().start()
        for k in wait:
            copy(k).wait_recv()
        for k in start:
            copy(k).start()
        if number == 0:
            into().start()
        if number == 4:
            for k in range(self.copies):
                copy(k).wait_send()
            out().wait()


class Spread:
    stages = 0

    def __init__(self, part):
        _, _, rows, columns = part.shape
        self.inputs = [part]
        self.outputs = [jax.ShapeDtypeStruct((2, rows // 2, columns), BF)] * 2
        self.scratch = [pltpu.SemaphoreType.DMA((2,)), pltpu.SemaphoreType.DMA((2,))]

    def pairs(self, at, ins, outs):
        (part,), (first, second) = ins, outs
        half = part.shape[2] // 2
        return [
            (part.at[1 - at.x, :, pl.ds(0, half), :], first, at.to_x),
            (part.at[:, 1 - at.y, pl.ds(half, half), :], second, at.to_y),
        ]

    def stage(self, at, number, ins, outs, scratch):
        for k, (src, dst, peer) in enumerate(self.pairs(at, ins, outs)):
            copy = remote(src, dst, scratch, k, peer)
            if number == 0:
                copy.start()
            else:
                copy.wait()


class Cross(Spread):
    def __init__(self, part):
        self.inputs = [part]
        self.outputs = [jax.ShapeDtypeStruct(part.shape, BF)]
        self.scratch = [pltpu.SemaphoreType.DMA((2,)), pltpu.SemaphoreType.DMA((2,))]

    def pairs(self, at, ins, outs):
        (part,), (got,) = ins, outs
        return [(part.at[0], got.at[0], at.to_y), (part.at[1], got.at[1], at.to_x)]


class Rise(Cross):
    def pairs(self, at, ins, outs):
        (part,), (got,) = ins, outs
        return [(part, got, at.to_z)]


def call(name, body, grid, ins, in_specs, outs, out_specs, scratch, comms, number, flops, points=None):
    n_in, n_out, n_scratch = len(ins), len(outs), len(scratch)
    steps = functools.reduce(lambda a, b: a * b, grid, 1)
    points = points or {}

    def kernel(*refs):
        refs = list(refs)
        take = lambda n: [refs.pop(0) for _ in range(n)]
        i_refs = take(n_in)
        ci = [take(len(m.inputs)) for m in comms]
        o_refs = take(n_out)
        co = [take(len(m.outputs)) for m in comms]
        s_refs = take(n_scratch)
        cs = [take(len(m.scratch)) for m in comms]
        at = Place()
        step = pl.program_id(0)
        if len(grid) == 2:
            step = step * grid[1] + pl.program_id(1)

        @pl.when(step == 0)
        def _():
            at.greet()
            for m, i, o, s in zip(comms, ci, co, cs):
                m.stage(at, 0, i, o, s)

        last = {}
        for index, m in enumerate(comms):
            for stage in range(1, m.stages):
                last.setdefault(min(points.get((index, stage), steps - 1), steps - 1), []).append((index, stage))
        for when, events in last.items():
            if when < steps - 1:

                @pl.when(step == when)
                def _(events=events):
                    for index, stage in events:
                        comms[index].stage(at, stage, ci[index], co[index], cs[index])

        body(at, step, i_refs, o_refs, s_refs)

        @pl.when(step == steps - 1)
        def _():
            late = last.get(steps - 1, [])
            for stage in range(1, Gather.stages):
                for index, wanted in late:
                    if wanted == stage:
                        comms[index].stage(at, stage, ci[index], co[index], cs[index])
            for m, i, o, s in zip(comms, ci, co, cs):
                m.stage(at, max(m.stages, 1), i, o, s)

    flat = lambda key: [v for m in comms for v in getattr(m, key)]
    moved = flat("inputs")
    results = pl.pallas_call(
        kernel,
        grid=grid,
        in_specs=list(in_specs) + [ANY] * len(moved),
        out_specs=list(out_specs) + [ANY] * len(flat("outputs")),
        out_shape=list(outs) + flat("outputs"),
        scratch_shapes=list(scratch) + flat("scratch"),
        compiler_params=pltpu.CompilerParams(
            collective_id=number,
            has_side_effects=True,
            vmem_limit_bytes=VMEM_LIMIT,
            dimension_semantics=("arbitrary",) * len(grid),
        ),
        cost_estimate=pl.CostEstimate(flops=flops, bytes_accessed=1 << 24, transcendentals=0),
        name=name,
    )(*ins, *moved)
    results = list(results)
    mine, results = results[:n_out], results[n_out:]
    got = []
    for m in comms:
        got.append(results[: len(m.outputs)])
        results = results[len(m.outputs) :]
    return mine, got


def scale_of(wide):
    return lax.rsqrt(jnp.mean(wide * wide, -1, keepdims=True) + 1e-6)


def shape(dims, dtype=BF):
    return jax.ShapeDtypeStruct(dims, dtype)


def once(dims, index):
    return pl.BlockSpec(dims, index, pipeline_mode=pl.Buffered(1))


def dot(a, b, ca=1, cb=0):
    return lax.dot_general(a, b, (((ca,), (cb,)), ((), ())), preferred_element_type=F32)


def first_norm(h, comms, number):
    def body(at, step, ins, outs, scratch):
        wide = ins[0][...].astype(F32)
        outs[0][...] = (wide * scale_of(wide)).astype(BF)

    tile = pl.BlockSpec((512, D), lambda i: (i, 0))
    (a,), got = call("fetch", body, (4,), [h], [tile], [shape((TOK, D))], [tile], [], comms, number, 10**7)
    return a, got


def gate_up(a, wg, wu, comms, number, points):
    rows, cols = 1024, 512

    def body(at, step, ins, outs, scratch):
        a_ref, g_ref, u_ref = ins
        act, gate, up = outs
        start = pl.program_id(1) * rows
        g_w = g_ref[...].reshape(D, cols)
        u_w = u_ref[...].reshape(D, cols)
        for k in range(rows // 512):
            part = pl.ds(k * 512, 512)
            left = a_ref[pl.ds(pl.multiple_of(start + k * 512, 512), 512), :]
            g = dot(left, g_w)
            u = dot(left, u_w)
            gate[part, :] = g
            up[part, :] = u
            act[part, :] = (g * jax.nn.sigmoid(g) * u).astype(BF)

    weight = pl.BlockSpec((8, 160, cols), lambda j, i: (0, 0, j))
    tile = pl.BlockSpec((rows, cols), lambda j, i: (i, j))
    return call(
        "gate_up", body, (FF // cols, TOK // rows), [a, wg, wu], [once((TOK, D), lambda j, i: (0, 0)), weight, weight],
        [shape((TOK, FF)), shape((TOK, FF), F32), shape((TOK, FF), F32)], [tile] * 3, [], comms, number, 4 * TOK * D * FF, points,
    )


def down(act, wd, h, comms, number, points):
    rows = 256

    def body(at, step, ins, outs, scratch):
        act_ref, w_ref, h_ref = ins
        out = dot(act_ref[...], w_ref[...].reshape(FF, D)).astype(BF)
        new = (h_ref[...].astype(F32) + out.astype(F32)).astype(BF)
        outs[0][...] = new
        wide = new.astype(F32)
        outs[1][...] = (wide * scale_of(wide)).astype(BF)

    tile = pl.BlockSpec((rows, D), lambda i: (i, 0))
    return call(
        "down", body, (TOK // rows,), [act, wd, h], [pl.BlockSpec((rows, FF), lambda i: (i, 0)), once((8, 384, D), lambda i: (0, 0, 0)), tile],
        [shape((TOK, D)), shape((TOK, D))], [tile, tile], [], comms, number, 2 * TOK * D * FF, points,
    )


def by_act(dy, wd, gate, up, comms, number):
    rows, cols = 512, 768

    def body(at, step, ins, outs, scratch):
        dy_ref, w_ref, g_ref, u_ref = ins
        left = dy_ref[pl.ds(pl.multiple_of(pl.program_id(1) * rows, rows), rows), :]
        da = dot(left, w_ref[...].reshape(cols, D), 1, 1).astype(BF).astype(F32)
        g, u = g_ref[...], u_ref[...]
        sig = jax.nn.sigmoid(g)
        silu = g * sig
        outs[0][0] = (da * u * (sig + silu * (1 - sig))).astype(BF)
        outs[0][1] = (da * silu).astype(BF)

    tile = pl.BlockSpec((rows, cols), lambda j, i: (i, j))
    return call(
        "by_act", body, (FF // cols, TOK // rows), [dy, wd, gate, up],
        [once((TOK, D), lambda j, i: (0, 0)), pl.BlockSpec((2, 384, D), lambda j, i: (j, 0, 0)), tile, tile],
        [shape((2, TOK, FF))], [pl.BlockSpec((2, rows, cols), lambda j, i: (0, i, j))], [], comms, number, 2 * TOK * D * FF,
    )


def by_state(dgu, wg, wu, h, dy, comms, number):
    rows = 256

    def body(at, step, ins, outs, scratch):
        d_ref, g_ref, u_ref, h_ref, dy_ref = ins
        first = dot(d_ref[0], g_ref[...].reshape(D, FF), 1, 1).astype(BF)
        second = dot(d_ref[1], u_ref[...].reshape(D, FF), 1, 1).astype(BF)
        da = (first.astype(F32) + second.astype(F32)).astype(BF).astype(F32)
        wide = h_ref[...].astype(F32)
        scale = scale_of(wide)
        along = jnp.sum(da * wide, -1, keepdims=True)
        dh = da * scale - wide * (along * scale * scale * scale * (1.0 / D))
        outs[0][...] = (dy_ref[...].astype(F32) + dh.astype(BF).astype(F32)).astype(BF)

    tile = pl.BlockSpec((rows, D), lambda i: (i, 0))
    weight = once((8, 160, FF), lambda i: (0, 0, 0))
    return call(
        "by_state", body, (TOK // rows,), [dgu, wg, wu, h, dy],
        [pl.BlockSpec((2, rows, FF), lambda i: (0, i, 0)), weight, weight, tile, tile],
        [shape((TOK, D))], [tile], [], comms, number, 4 * TOK * D * FF,
    )


def by_down(act, dy, comms, number):
    n = 4

    def body(at, step, ins, outs, scratch):
        act_ref, dy_ref = ins
        term, mine, send, recv, *sems = scratch

        def copy(t, slot):
            return remote(send.at[slot], recv.at[t], sems, t, at.to_sib)

        @pl.when(step > 0)
        def _():
            copy(step - 1, (step - 1) % 2).wait_recv()
            total = mine[...].astype(F32) + recv[step - 1].astype(F32)
            outs[0][0] = total.astype(BF)
            outs[1][0] = total

        @pl.when(step < n)
        def _():
            @pl.when(step > 1)
            def _():
                copy(step - 2, step % 2).wait_send()

            for k in range(2):
                term[k] = dot(act_ref[:, k * 384 : (k + 1) * 384], dy_ref[...], 0, 0).astype(BF)
            send[step % 2] = term[1 - at.c]
            mine[...] = term[at.c]
            copy(step, step % 2).start()

        @pl.when(step == n)
        def _():
            copy(n - 2, n % 2).wait_send()
            copy(n - 1, (n - 1) % 2).wait_send()

    before = lambda i: (jnp.maximum(i - 1, 0), 0, 0)
    out = pl.BlockSpec((1, 384, D), before)
    return call(
        "by_down", body, (n + 1,), [act, dy],
        [pl.BlockSpec((TOK, 768), lambda i: (0, jnp.minimum(i, n - 1))), once((TOK, D), lambda i: (0, 0))],
        [shape((n, 384, D)), shape((n, 384, D), F32)], [out, out],
        [pltpu.VMEM((2, 384, D), BF), pltpu.VMEM((384, D), BF), pltpu.VMEM((2, 384, D), BF), pltpu.VMEM((n, 384, D), BF),
         pltpu.SemaphoreType.DMA((n,)), pltpu.SemaphoreType.DMA((n,))],
        comms, number, 2 * TOK * D * FF,
    )


def by_gate_up(a, dgu, comms, number):
    cols = 512
    each = FF // cols
    n = 2 * each

    def body(at, step, ins, outs, scratch):
        a_ref, d_ref = ins
        across, term, mine, send, recv, *sems = scratch

        def copy(t, slot):
            return remote(send.at[slot], recv.at[t], sems, t, at.to_sib)

        @pl.when(step == 0)
        def _():
            for k in range(TOK // 256):
                across[:, k * 256 : (k + 1) * 256] = a_ref[k * 256 : (k + 1) * 256, :].T

        @pl.when(step > 0)
        def _():
            copy(step - 1, (step - 1) % 2).wait_recv()
            total = mine[...].astype(F32) + recv[step - 1].astype(F32)
            outs[0][:, 0] = total.astype(BF)
            outs[1][:, 0] = total

        @pl.when(step < n)
        def _():
            @pl.when(step > 1)
            def _():
                copy(step - 2, step % 2).wait_send()

            term[...] = dot(across[...], d_ref[0]).astype(BF).reshape(8, 160, cols)
            for k in range(4):
                send[step % 2, k] = term[2 * k + 1 - at.c]
                mine[k] = term[2 * k + at.c]
            copy(step, step % 2).start()

        @pl.when(step == n)
        def _():
            copy(n - 2, n % 2).wait_send()
            copy(n - 1, (n - 1) % 2).wait_send()

    def before(i):
        t = jnp.maximum(i - 1, 0)
        return 0, t // each, 0, t % each

    def now(i):
        t = jnp.minimum(i, n - 1)
        return t // each, 0, t % each

    out = pl.BlockSpec((4, 1, 160, cols), before)
    return call(
        "by_gate_up", body, (n + 1,), [a, dgu], [once((TOK, D), lambda i: (0, 0)), pl.BlockSpec((1, TOK, cols), now)],
        [shape((4, 2, 160, FF)), shape((4, 2, 160, FF), F32)], [out, out],
        [pltpu.VMEM((D, TOK), BF), pltpu.VMEM((8, 160, cols), BF), pltpu.VMEM((4, 160, cols), BF), pltpu.VMEM((2, 4, 160, cols), BF),
         pltpu.VMEM((n, 4, 160, cols), BF), pltpu.SemaphoreType.DMA((n,)), pltpu.SemaphoreType.DMA((n,))],
        comms, number, 4 * TOK * D * FF,
    )


def only(comms, number):
    def body(at, step, ins, outs, scratch):
        outs[0][...] = jnp.zeros((8, 128), F32)

    tile = pl.BlockSpec((8, 128), lambda i: (0, 0))
    return call("exchange", body, (1,), [], [], [shape((8, 128), F32)], [tile], [], comms, number, 10**6)[1]


class Sum:
    def __init__(self, at, part, wide, rows, columns):
        self.at, self.rows = at, rows
        self.part, self.wide = part.reshape(2, 2, rows, columns), wide.reshape(2, 2, rows, columns)

    def pick(self, x, y, second):
        half = self.rows // 2
        block = lax.dynamic_slice(self.wide, (x, y, half * second, 0), (1, 1, half, self.wide.shape[3]))
        return block[0, 0]

    def spread(self):
        return Spread(self.part)

    def cross(self, got):
        self.a, self.b = got
        at = self.at
        low = self.pick(at.x, 1 - at.y, 0) + lax.dynamic_index_in_dim(self.a, 1 - at.y, 0, False).astype(F32)
        high = self.pick(1 - at.x, at.y, 1) + lax.dynamic_index_in_dim(self.b, 1 - at.x, 0, False).astype(F32)
        return Cross(jnp.stack([low, high]).astype(BF))

    def rise(self, got):
        (c,) = got
        at = self.at
        low = self.pick(at.x, at.y, 0) + lax.dynamic_index_in_dim(self.a, at.y, 0, False).astype(F32) + c[0].astype(F32)
        high = self.pick(at.x, at.y, 1) + lax.dynamic_index_in_dim(self.b, at.x, 0, False).astype(F32) + c[1].astype(F32)
        self.total = jnp.stack([low, high])
        return self.total.astype(BF)

    def end(self, got):
        return (self.total + got.astype(F32)).astype(BF)


def solution(mesh):
    def step(x, dy, w_gate, w_up, w_down):
        x, dy = x[0], dy[0]
        at = Place()
        g, u, d = ([w[0], w[1]] for w in (w_gate, w_up, w_down))
        a0, ((g0,), (u0,)) = first_norm(x, [Gather(g[0]), Gather(u[0])], 0)
        points = {(0, 1): 5, (0, 2): 9, (1, 1): 9}
        (act0, gate0, up0), ((d0,), (g1,)) = gate_up(a0, g0, u0, [Gather(d[0]), Gather(g[1])], 1, points)
        (h1, a1), ((u1,),) = down(act0, d0, x, [Gather(u[1])], 2, {(0, 1): 6})
        (act1, gate1, up1), ((d1,),) = gate_up(a1, g1, u1, [Gather(d[1])], 3, {(0, 1): 5, (0, 2): 8, (0, 3): 10})

        def sums(pair, rows, columns):
            return Sum(at, *pair, rows, columns)

        pair, _ = by_down(act1, dy, [], 4)
        s_d1 = sums(pair, 384, D)
        (dgu1,), (got,) = by_act(dy, d1, gate1, up1, [s_d1.spread()], 5)
        pair, (got,) = by_gate_up(a1, dgu1, [s_d1.cross(got)], 6)
        s_gu1 = sums(pair, 320, FF)
        (dh1,), (got, (z_d1,)) = by_state(dgu1, g1, u1, h1, dy, [s_gu1.spread(), Rise(s_d1.rise(got))], 7)
        pair, (got,) = by_down(act0, dh1, [s_gu1.cross(got)], 8)
        s_d0 = sums(pair, 384, D)
        up_gu1 = s_gu1.rise(got)
        (dgu0,), (got, (z_g1,)) = by_act(dh1, d0, gate0, up0, [s_d0.spread(), Rise(up_gu1[0])], 9)
        pair, (got, (z_u1,)) = by_gate_up(a0, dgu0, [s_d0.cross(got), Rise(up_gu1[1])], 10)
        s_gu0 = sums(pair, 320, FF)
        (dx,), (got, (z_d0,)) = by_state(dgu0, g0, u0, x, dh1, [s_gu0.spread(), Rise(s_d0.rise(got))], 11)
        (got,) = only([s_gu0.cross(got)], 12)
        up_gu0 = s_gu0.rise(got)
        ((z_gu0,),) = only([Rise(up_gu0)], 13)

        gu1 = s_gu1.end(jnp.stack([z_g1, z_u1]))
        gu0 = s_gu0.end(z_gu0)
        down1, down0 = s_d1.end(z_d1).reshape(384, D), s_d0.end(z_d0).reshape(384, D)
        return dx[None], jnp.stack([gu0[0], gu1[0]]), jnp.stack([gu0[1], gu1[1]]), jnp.stack([down0, down1])

    states, cut = P(("rep", "r", "s"), None, None), P(None, "s", None)
    return jax.shard_map(
        step,
        mesh=mesh,
        in_specs=(states, states) + (cut,) * 3,
        out_specs=(states,) + (P("rep", "s", None),) * 3,
        check_vma=False,
    )
```

```python
import functools

import jax
import jax.numpy as jnp
from jax import lax
from jax.experimental import pallas as pl
from jax.experimental.pallas import tpu as pltpu
from jax.sharding import PartitionSpec as P

MESH = pl.DeviceIdType.MESH
END = (1 << 30, 99)
BF, F32 = jnp.bfloat16, jnp.float32
ANY = pl.BlockSpec(memory_space=pl.ANY)
VMEM_LIMIT = 66_000_000
TOK, D, FF = 2048, 1280, 3072


class Place:
    def __init__(self):
        self.z = lax.axis_index("r")
        self.s = lax.axis_index("s")
        self.x = self.s // 4
        self.y = (self.s // 2) % 2
        self.c = self.s % 2
        self.xs = self.s + 4 - 8 * self.x
        self.ys = self.s + 2 - 4 * self.y
        self.sib = self.s + 1 - 2 * self.c
        self.ds = self.xs + 2 - 4 * self.y
        self.to_x, self.to_y, self.to_sib = {"s": self.xs}, {"s": self.ys}, {"s": self.sib}
        self.to_z = {"r": 1 - self.z}

    def greet(self):
        barrier = pltpu.get_barrier_semaphore()
        for peer in (self.to_x, self.to_y, self.to_sib, self.to_z):
            pl.semaphore_signal(barrier, inc=1, device_id=peer, device_id_type=MESH)
        pl.semaphore_wait(barrier, 4)


def remote(src, dst, sems, k, peer):
    return pltpu.make_async_remote_copy(
        src_ref=src, dst_ref=dst, send_sem=sems[0].at[k], recv_sem=sems[1].at[k], device_id=peer, device_id_type=MESH
    )


class Gather:
    copies = 14
    last = 4

    def __init__(self, whole, layer, blocks=1, only=None, onto=None):
        self.inputs, self.layer, self.blocks = [whole] + ([] if onto is None else [onto]), layer, blocks
        self.listed, self.goes_on = range(blocks) if only is None else only, onto is not None
        dims = whole.shape[1:]
        self.outputs = [jax.ShapeDtypeStruct((8, *dims), whole.dtype)]
        self.scratch = [
            pltpu.VMEM(dims, whole.dtype),
            pltpu.SemaphoreType.DMA((2,)),
            pltpu.SemaphoreType.DMA((self.copies * blocks,)),
            pltpu.SemaphoreType.DMA((self.copies * blocks,)),
        ]

    def stage(self, at, number, ins, outs, scratch, c=0):
        (whole, *_), (full,), (held, local, *sems) = ins, outs, scratch
        own = whole.at[self.layer]
        rows = own.shape[0]
        width = own.shape[1] // self.blocks
        cols = pl.ds(c * width, width)
        low = 48 if rows == 160 else rows // 3
        both = rows - low
        everything = pl.ds(0, rows)
        plane = pl.ds(pl.multiple_of(at.z * low, 16), both)
        middle = pl.ds(low, both - low)
        mine = pl.ds(pl.multiple_of(at.z * both, 16), low)
        theirs = pl.ds(pl.multiple_of((1 - at.z) * both, 16), low)

        def copy(k):
            def again(s, r, peer):
                return full.at[s, r, cols], full.at[s, r, cols], peer

            src, dst, peer = {
                0: lambda: (own.at[plane, cols], full.at[at.s, plane, cols], at.to_x),
                1: lambda: (own.at[plane, cols], full.at[at.s, plane, cols], at.to_y),
                2: lambda: (own.at[everything, cols], full.at[at.s, everything, cols], at.to_sib),
                3: lambda: again(at.xs, middle, at.to_y),
                4: lambda: again(at.ys, mine, at.to_x),
                5: lambda: again(at.xs, mine, at.to_z),
                6: lambda: again(at.ys, mine, at.to_z),
                7: lambda: again(at.xs, plane, at.to_sib),
                8: lambda: again(at.ys, plane, at.to_sib),
                9: lambda: again(at.ds, mine, at.to_z),
                10: lambda: again(at.ds, plane, at.to_sib),
                11: lambda: again(at.xs, theirs, at.to_sib),
                12: lambda: again(at.ys, theirs, at.to_sib),
                13: lambda: again(at.ds, theirs, at.to_sib),
            }[k]()
            return remote(src, dst, sems, self.copies * c + k, peer)

        into = lambda: pltpu.make_async_copy(own, held, local.at[0])
        out = lambda: pltpu.make_async_copy(held, full.at[at.s], local.at[1])
        wait, start = {
            0: ((), (0, 1, 2)),
            1: ((0, 1), (3, 4, 5, 6, 7, 8)),
            2: ((3, 4), (9, 10)),
            3: ((5, 6, 9), (11, 12, 13)),
            4: ((2, 7, 8, 10, 11, 12, 13), ()),
        }[number]
        own_too = c == self.listed[0] and not self.goes_on
        if number == 1 and own_too:
            into().wait()
            out().start()
        for k in wait:
            copy(k).wait_recv()
        for k in start:
            copy(k).start()
        if number == 0 and own_too:
            into().start()
        if number == 4:
            for k in range(self.copies):
                copy(k).wait_send()
            if own_too:
                out().wait()


class Cross:
    blocks, last = 1, 1

    def __init__(self, part):
        self.inputs = [part]
        self.outputs = [jax.ShapeDtypeStruct(part.shape, BF)]
        self.scratch = [pltpu.SemaphoreType.DMA((2,)), pltpu.SemaphoreType.DMA((2,))]

    def pairs(self, at, ins, outs):
        (part,), (got,) = ins, outs
        half = part.shape[1] // 2
        low, high = pl.ds(0, half), pl.ds(half, half)
        return [(part.at[:, low, :], got.at[:, low, :], at.to_y), (part.at[:, high, :], got.at[:, high, :], at.to_x)]

    def stage(self, at, number, ins, outs, scratch, c=0):
        for k, (src, dst, peer) in enumerate(self.pairs(at, ins, outs)):
            copy = remote(src, dst, scratch, k, peer)
            if number == 0:
                copy.start()
            else:
                copy.wait()


class Rise(Cross):
    def pairs(self, at, ins, outs):
        (part,), (got,) = ins, outs
        return [(part, got, at.to_z)]


class Spread(Cross):
    def __init__(self, to_x, to_y):
        _, half, columns = to_x.shape
        self.inputs = [to_x, to_y]
        self.outputs = [jax.ShapeDtypeStruct((2, 2 * half, columns), BF)]
        self.scratch = [pltpu.SemaphoreType.DMA((2,)), pltpu.SemaphoreType.DMA((2,))]

    def pairs(self, at, ins, outs):
        (to_x, to_y), (got,) = ins, outs
        half = to_x.shape[1]
        return [(to_x, got.at[:, pl.ds(0, half), :], at.to_x), (to_y, got.at[:, pl.ds(half, half), :], at.to_y)]


class Chain:
    blocks, last = 2, 4

    def __init__(self, kept, to_x, to_y):
        _, rows, columns = kept.shape
        self.inputs = [kept, to_x, to_y]
        self.outputs = [jax.ShapeDtypeStruct((rows, columns), BF)]
        self.cut = columns // 2
        one, two = (2, rows, self.cut), (2, 2, rows, self.cut)
        self.scratch = [pltpu.VMEM(two, F32), pltpu.VMEM(two, BF)] + [pltpu.VMEM(one, BF)] * 4
        self.scratch += [pltpu.SemaphoreType.DMA((2, 5)), pltpu.SemaphoreType.DMA((2, 5)), pltpu.SemaphoreType.DMA((2, 2))]

    def stage(self, at, number, ins, outs, scratch, c=0):
        (kept, to_x, to_y), (result,), (base, far, ahead, second, sent, third, *sems, local) = ins, outs, scratch
        rows = kept.shape[1]
        half = rows // 2
        cols = pl.ds(c * self.cut, self.cut)
        low, high = pl.ds(0, half), pl.ds(half, half)

        def send(k):
            src, dst, peer = {
                0: lambda: (to_x.at[:, :, cols], far.at[c, :, low, :], at.to_x),
                1: lambda: (to_y.at[:, :, cols], far.at[c, :, high, :], at.to_y),
                2: lambda: (ahead.at[c, low, :], second.at[c, low, :], at.to_y),
                3: lambda: (ahead.at[c, high, :], second.at[c, high, :], at.to_x),
                4: lambda: (sent.at[c], third.at[c], at.to_z),
            }[k]()
            return pltpu.make_async_remote_copy(
                src_ref=src, dst_ref=dst, send_sem=sems[0].at[c, k], recv_sem=sems[1].at[c, k], device_id=peer, device_id_type=MESH
            )

        load = lambda: pltpu.make_async_copy(kept.at[:, :, cols], base.at[c], local.at[c, 0])
        store = lambda: pltpu.make_async_copy(sent.at[c], result.at[:, cols], local.at[c, 1])

        def each(f):
            @pl.loop(0, rows // 16)
            def _(k):
                f(pl.ds(pl.multiple_of(k * 16, 16), 16))

        if number == 0:
            for copy in (send(0), send(1), load()):
                copy.start()
        elif number == 1:
            for copy in (send(0), send(1), load()):
                copy.wait()

            def f(r):
                ahead[c, r, :] = (base[c, 1, r, :] + far[c, 1, r, :].astype(F32)).astype(BF)

            each(f)
            send(2).start()
            send(3).start()
        elif number == 2:
            send(2).wait()
            send(3).wait()

            def f(r):
                new = base[c, 0, r, :] + far[c, 0, r, :].astype(F32) + second[c, r, :].astype(F32)
                base[c, 0, r, :] = new
                sent[c, r, :] = new.astype(BF)

            each(f)
            send(4).start()
        elif number == 3:
            send(4).wait()

            def f(r):
                sent[c, r, :] = (base[c, 0, r, :] + third[c, r, :].astype(F32)).astype(BF)

            each(f)
            store().start()
        else:
            store().wait()


class Finish:
    last = 3

    def __init__(self, part, kept, far):
        mats, rows, columns = part.shape
        self.inputs = [part, kept, far]
        self.outputs = [jax.ShapeDtypeStruct(part.shape, BF)]
        self.blocks, self.cut = 2 * mats, columns // 2
        each = (self.blocks, rows, self.cut)
        n = self.blocks
        self.scratch = [pltpu.VMEM(each, F32)] + [pltpu.VMEM(each, BF)] * 4
        self.scratch += [pltpu.SemaphoreType.DMA((n, 3)), pltpu.SemaphoreType.DMA((n, 3)), pltpu.SemaphoreType.DMA((n, 3))]

    def stage(self, at, number, ins, outs, scratch, c=0):
        (part, kept, far), (result,), (total, first, second, sent, third, *sems, local) = ins, outs, scratch
        rows = part.shape[1]
        half = rows // 2
        m, cols = c // 2, pl.ds(c % 2 * self.cut, self.cut)
        low, high = pl.ds(0, half), pl.ds(half, half)

        def along(k):
            r, peer = ((low, at.to_y), (high, at.to_x))[k]
            return pltpu.make_async_remote_copy(
                src_ref=part.at[m, r, cols], dst_ref=second.at[c, r, :], send_sem=sems[0].at[c, k], recv_sem=sems[1].at[c, k],
                device_id=peer, device_id_type=MESH,
            )

        def up():
            return pltpu.make_async_remote_copy(
                src_ref=sent.at[c], dst_ref=third.at[c], send_sem=sems[0].at[c, 2], recv_sem=sems[1].at[c, 2],
                device_id=at.to_z, device_id_type=MESH,
            )

        def loads():
            return [
                pltpu.make_async_copy(kept.at[0, m, :, cols], total.at[c], local.at[c, 0]),
                pltpu.make_async_copy(far.at[0, m, :, cols], first.at[c], local.at[c, 1]),
            ]

        def store():
            return pltpu.make_async_copy(sent.at[c], result.at[m, :, cols], local.at[c, 2])

        def each(f):
            @pl.loop(0, rows // 16)
            def _(k):
                f(pl.ds(pl.multiple_of(k * 16, 16), 16))

        if number == 0:
            for copy in (along(0), along(1), *loads()):
                copy.start()
        elif number == 1:
            for copy in (along(0), along(1), *loads()):
                copy.wait()

            def f(r):
                new = total[c, r, :] + first[c, r, :].astype(F32) + second[c, r, :].astype(F32)
                total[c, r, :] = new
                sent[c, r, :] = new.astype(BF)

            each(f)
            up().start()
        elif number == 2:
            up().wait()

            def f(r):
                sent[c, r, :] = (total[c, r, :] + third[c, r, :].astype(F32)).astype(BF)

            each(f)
            store().start()
        else:
            store().wait()


def call(name, body, grid, ins, in_specs, outs, out_specs, scratch, comms, number, flops, points=None):
    n_in, n_out, n_scratch = len(ins), len(outs), len(scratch)
    steps = functools.reduce(lambda a, b: a * b, grid, 1)
    points = points or {}
    events = {}
    for index, m in enumerate(comms):
        for c in getattr(m, 'listed', range(m.blocks)):
            for stage in range(m.last + 1):
                when = points.get((index, c, stage), 0 if stage == 0 else steps)
                when = when if isinstance(when, tuple) else (when, 0)
                events.setdefault(when if when[0] < steps else END, []).append((stage == 0, c, stage, index))

    def kernel(*refs):
        refs = list(refs)
        take = lambda n: [refs.pop(0) for _ in range(n)]
        i_refs = take(n_in)
        ci = [take(len(m.inputs)) for m in comms]
        o_refs = take(n_out)
        co = [take(len(m.outputs)) for m in comms]
        s_refs = take(n_scratch)
        cs = [take(len(m.scratch)) for m in comms]
        at = Place()
        step = pl.program_id(0)
        if len(grid) == 2:
            step = step * grid[1] + pl.program_id(1)

        @pl.when(step == 0)
        def _():
            at.greet()

        def happen(sub):
            for when, listed in events.items():
                if when[1] == sub:
                    order = sorted(listed, key=lambda e: (e[2], e[1], e[3])) if when == END else sorted(listed)

                    @pl.when(step == (steps - 1 if when == END else when[0]))
                    def _(order=order):
                        for _, c, stage, index in order:
                            comms[index].stage(at, stage, ci[index], co[index], cs[index], c)

        happen(0)
        body(at, step, i_refs, o_refs, s_refs, (co, happen))
        happen(END[1])

    flat = lambda key: [v for m in comms for v in getattr(m, key)]
    moved = flat("inputs")
    aliases, i, o = {}, n_in, n_out
    for m in comms:
        if getattr(m, "goes_on", False):
            aliases[i + 1] = o
        i, o = i + len(m.inputs), o + len(m.outputs)
    results = pl.pallas_call(
        kernel,
        grid=grid,
        in_specs=list(in_specs) + [ANY] * len(moved),
        out_specs=list(out_specs) + [ANY] * len(flat("outputs")),
        out_shape=list(outs) + flat("outputs"),
        scratch_shapes=list(scratch) + flat("scratch"),
        compiler_params=pltpu.CompilerParams(
            collective_id=number,
            has_side_effects=True,
            vmem_limit_bytes=VMEM_LIMIT,
            dimension_semantics=("arbitrary",) * len(grid),
        ),
        cost_estimate=pl.CostEstimate(flops=flops, bytes_accessed=1 << 24, transcendentals=0),
        name=name,
        input_output_aliases=aliases,
    )(*ins, *moved)
    results = list(results)
    mine, results = results[:n_out], results[n_out:]
    got = []
    for m in comms:
        got.append(results[: len(m.outputs)])
        results = results[len(m.outputs) :]
    return mine, got


def scale_of(wide):
    return lax.rsqrt(jnp.mean(wide * wide, -1, keepdims=True) + 1e-6)


def shape(dims, dtype=BF):
    return jax.ShapeDtypeStruct(dims, dtype)


def once(dims, index):
    return pl.BlockSpec(dims, index, pipeline_mode=pl.Buffered(1))


def dot(a, b, ca=1, cb=0):
    return lax.dot_general(a, b, (((ca,), (cb,)), ((), ())), preferred_element_type=F32)


def load_block(landed, buffers, sems, c, width):
    cols = pl.ds(c * width if isinstance(c, int) else pl.multiple_of(c * width, width), width)
    return [pltpu.make_async_copy(landed[m][0].at[:, :, cols], buffers.at[c % 2, m], sems.at[c % 2, m]) for m in range(2)]


def gate_up(x, w_gate, w_up, w_down, number):
    cols, blocks, lag = 512, FF // 512, 5

    def body(at, step, ins, outs, scratch, landed):
        x_ref = ins[0]
        a_out, act, gate, up = outs
        held, sems = scratch

        @pl.when(step == 0)
        def _():
            for k in range(TOK // 512):
                part = pl.ds(k * 512, 512)
                wide = x_ref[part, :].astype(F32)
                a_out[part, :] = (wide * scale_of(wide)).astype(BF)

        def load(c):
            for copy in load_block(arrived, held, sems, c, cols):
                copy.start()

        arrived, happen = landed

        @pl.when(step == lag - 1)
        def _():
            load(0)

        c = jnp.maximum(step - lag, 0)

        @pl.when(step >= lag)
        def _():
            for copy in load_block(arrived, held, sems, c, cols):
                copy.wait()

        for k in range(4):
            if k:
                happen(k)
            if k == 3:

                @pl.when((step >= lag) & (step < lag + blocks - 1))
                def _():
                    load(c + 1)

            @pl.when(step >= lag)
            def _(k=k):
                part = pl.ds(k * 512, 512)
                left = a_out[part, :]
                g = dot(left, held[c % 2, 0].reshape(D, cols))
                u = dot(left, held[c % 2, 1].reshape(D, cols))
                gate[part, :] = g
                up[part, :] = u
                act[part, :] = (g * jax.nn.sigmoid(g) * u).astype(BF)

    tile = pl.BlockSpec((TOK, cols), lambda i: (0, jnp.maximum(i - lag, 0)))
    whole = once((TOK, D), lambda i: (0, 0))
    comms = [Gather(w_gate, 0, blocks), Gather(w_up, 0, blocks), Gather(w_down, 0, 2)]
    when = {(0, k): k for k in range(5)} | {(1, 0): 1, (1, 1): lag - 1, (2, 0): lag - 1}
    for c in range(1, blocks + 1):
        rest = {(c + 1, 0): (lag + c - 2, 2), (c, 1): (lag + c - 2, 2), (c, 2): lag + c - 1, (c, 3): (lag + c - 1, 2), (c, 4): (lag + c - 1, 3)}
        when = rest | when
    points = {(m, c, k): when[c, k] for m in range(2) for c in range(blocks) for k in range(5)}
    points |= {(2, c, k): when[blocks - 1 + c, k] for c in range(2) for k in range(4)}
    return call(
        "gate_up", body, (blocks + lag,), [x], [whole], [shape((TOK, D)), shape((TOK, FF)), shape((TOK, FF), F32), shape((TOK, FF), F32)],
        [whole, tile, tile, tile], [pltpu.VMEM((2, 2, 8, 160, cols), BF), pltpu.SemaphoreType.DMA((2, 2))], comms, number, 4 * TOK * D * FF, points,
    )


def down(act, wd, h, comms, number, points):
    rows = 256

    def body(at, step, ins, outs, scratch, landed):
        act_ref, w_ref, h_ref = ins
        out = dot(act_ref[...], w_ref[...].reshape(FF, D)).astype(BF)
        new = (h_ref[...].astype(F32) + out.astype(F32)).astype(BF)
        outs[0][...] = new
        wide = new.astype(F32)
        outs[1][...] = (wide * scale_of(wide)).astype(BF)

    tile = pl.BlockSpec((rows, D), lambda i: (i, 0))
    return call(
        "down", body, (TOK // rows,), [act, wd, h], [pl.BlockSpec((rows, FF), lambda i: (i, 0)), once((8, 384, D), lambda i: (0, 0, 0)), tile],
        [shape((TOK, D)), shape((TOK, D))], [tile, tile], [], comms, number, 2 * TOK * D * FF, points,
    )


def middle(a, dy, wd, saved, weights, comms, number, extra=None):
    cols, rows = 768, 512
    blocks, tiles, n = FF // cols, TOK // rows, 2 * (FF // cols)
    lead = 1 if weights else 0
    steps = lead + blocks * tiles + 1
    across = TOK // tiles

    def body(at, step, ins, outs, scratch, landed):
        a_ref, dy_ref, wd_ref, *ins = ins
        d_out, kept, far, *outs = outs
        d_all, term, mine, send, recv, to_x, to_y, *sems = scratch
        t = step - lead
        j, i = t // tiles, t % tiles
        arrived, happen = landed

        def copy(u):
            return remote(send.at[u % 2], recv.at[u % 4], [s for s in sems[0:2]], u, at.to_sib)

        def there(u, half):
            return far.at[:, u % 2, pl.ds(80 * half, 80), pl.ds(pl.multiple_of(u // 2 * cols, cols), cols)]

        def along_x(u):
            return remote(to_x.at[u % 2], there(u, 0), sems[2:4], u, at.to_x)

        def along_y(u):
            return remote(to_y.at[u % 2], there(u, 1), sems[4:6], u, at.to_y)

        def finish(u):
            @pl.when(u > 1)
            def _():
                along_x(u - 2).wait_send()
                along_y(u - 2).wait_send()

            copy(u).wait_recv()
            slot = u % 2
            total = [mine[slot, k].astype(F32) + recv[u % 4, k].astype(F32) for k in range(4)]
            to_x[slot, 0] = total[0][:80].astype(BF)
            to_x[slot, 1] = total[1][:80].astype(BF)
            to_y[slot, 0] = total[2][80:].astype(BF)
            to_y[slot, 1] = total[1][80:].astype(BF)
            kept[0, 0] = total[3]
            kept[1, 0, :80] = total[2][:80]
            kept[1, 0, 80:] = total[0][80:]
            along_x(u).start()
            along_y(u).start()

        if weights:
            held, loads = scratch[-2:]

            @pl.when(step == lead - 1)
            def _():
                for load in load_block(arrived, held, loads, 0, cols):
                    load.start()

            @pl.when((t >= 0) & (t < blocks * tiles) & (i == 0))
            def _():
                for load in load_block(arrived, held, loads, j, cols):
                    load.wait()

        @pl.when((t >= 0) & (t < blocks * tiles))
        def _():
            sub = 256
            w = wd_ref[...].reshape(cols, D)
            for k in range(rows // sub):
                here = pl.ds(k * sub, sub)
                if weights:
                    left = a_ref[pl.ds(pl.multiple_of(i * rows + k * sub, sub), sub), :]
                    g = dot(left, held[j % 2, 0].reshape(D, cols))
                    u = dot(left, held[j % 2, 1].reshape(D, cols))
                else:
                    g, u = ins[0][here, :], ins[1][here, :]
                da = dot(dy_ref[here, :], w, 1, 1).astype(BF).astype(F32)
                sig = jax.nn.sigmoid(g)
                silu = g * sig
                if weights:
                    outs[0][here, :] = (silu * u).astype(BF)
                d_gate = (da * u * (sig + silu * (1 - sig))).astype(BF)
                d_up = (da * silu).astype(BF)
                d_out[0, here, :] = d_gate
                d_out[1, here, :] = d_up
                to = pl.ds(pl.multiple_of(i * rows + k * sub, sub), sub)
                d_all[0, to, :] = d_gate
                d_all[1, to, :] = d_up

        @pl.when((t > 0) & (i == 0))
        def _():
            finish(2 * j - 1)

        happen(1)

        for m in range(2):
            if m:
                happen(2)

            @pl.when((t >= 0) & (t < blocks * tiles) & (i == tiles - 1))
            def _(m=m):
                u = 2 * j + m

                @pl.when(u > 1)
                def _():
                    copy(u - 2).wait_send()

                term[...] = dot(a_ref[...], d_all[m], 0, 0).astype(BF).reshape(8, 160, cols)
                for k in range(4):
                    send[m, k] = term[2 * place(at, k) + 1 - at.c]
                    mine[m, k] = term[2 * place(at, k) + at.c]
                copy(u).start()
                if m:
                    finish(2 * j)

        happen(3)
        if weights:

            @pl.when((t >= 0) & (t < (blocks - 1) * tiles) & (i == tiles - 1))
            def _():
                for load in load_block(arrived, held, loads, j + 1, cols):
                    load.start()

        @pl.when(step == steps - 1)
        def _():
            for u in (n - 2, n - 1):
                copy(u).wait_send()
                along_x(u).wait_send()
                along_y(u).wait_send()

            @pl.loop(0, n)
            def _(u):
                along_x(u).wait_recv()
                along_y(u).wait_recv()

    def block(s):
        t = jnp.clip(s - lead, 0, blocks * tiles - 1)
        return t // tiles, t % tiles

    def done(s):
        t = jnp.maximum(s - lead, 0)
        late = t % tiles == tiles - 1
        early = t < tiles - 1
        return 0, jnp.where(late | early, 0, 1), 0, jnp.where(late, t // tiles, jnp.maximum(t // tiles - 1, 0))

    tile = pl.BlockSpec((rows, cols), lambda s: (block(s)[1], block(s)[0]))
    sems = lambda: pltpu.SemaphoreType.DMA((n,))
    ins = [a, dy, wd] + (list(saved) if saved else [])
    in_specs = [once((TOK, D), lambda s: (0, 0)), pl.BlockSpec((rows, D), lambda s: (block(s)[1], 0)), pl.BlockSpec((2, 384, D), lambda s: (block(s)[0], 0, 0))]
    in_specs += [tile, tile] if saved else []
    scratch = [
        pltpu.VMEM((2, TOK, cols), BF), pltpu.VMEM((8, 160, cols), BF), pltpu.VMEM((2, 4, 160, cols), BF), pltpu.VMEM((2, 4, 160, cols), BF),
        pltpu.VMEM((4, 4, 160, cols), BF), pltpu.VMEM((2, 2, 80, cols), BF), pltpu.VMEM((2, 2, 80, cols), BF),
    ] + [sems() for _ in range(6)]
    points = extra
    if weights:
        comms = [Gather(w, 1, blocks, (1, 2, 3), begun) for w, begun in weights] + comms
        scratch += [pltpu.VMEM((2, 2, 8, 160, cols), BF), pltpu.SemaphoreType.DMA((2, 2))]
        when = {1: (0, 4, (4, 2), (4, 3), (4, 3)), 2: (0, (4, 2), 5, 6, 7), 3: ((4, 2), 7, 8, (8, 1), (8, 2))}
        points = {(m, c, k): when[c][k] for m in range(2) for c in when for k in range(5)}
    outs = [shape((2, TOK, FF)), shape((2, 2, 160, FF), F32), shape((2, 2, 160, FF))] + ([shape((TOK, FF))] if weights else [])
    out_specs = [
        pl.BlockSpec((2, rows, cols), lambda s: (0, block(s)[1], block(s)[0])), pl.BlockSpec((2, 1, 160, cols), done), ANY,
    ] + ([tile] if weights else [])
    (dgu, kept, far, *act), got = call(
        "middle", body, (steps,), ins, in_specs, outs, out_specs, scratch, comms, number, (10 if weights else 6) * TOK * D * FF, points,
    )
    return dgu, Sum(kept, far), act, got


def by_state(dgu, wg, wu, h, dy, comms, number, points=None):
    rows = 256

    def body(at, step, ins, outs, scratch, landed):
        d_ref, g_ref, u_ref, h_ref, dy_ref = ins
        first = dot(d_ref[0], g_ref[...].reshape(D, FF), 1, 1).astype(BF)
        second = dot(d_ref[1], u_ref[...].reshape(D, FF), 1, 1).astype(BF)
        da = (first.astype(F32) + second.astype(F32)).astype(BF).astype(F32)
        wide = h_ref[...].astype(F32)
        scale = scale_of(wide)
        along = jnp.sum(da * wide, -1, keepdims=True)
        dh = da * scale - wide * (along * scale * scale * scale * (1.0 / D))
        outs[0][...] = (dy_ref[...].astype(F32) + dh.astype(BF).astype(F32)).astype(BF)

    tile = pl.BlockSpec((rows, D), lambda i: (i, 0))
    weight = once((8, 160, FF), lambda i: (0, 0, 0))
    return call(
        "by_state", body, (TOK // rows,), [dgu, wg, wu, h, dy],
        [pl.BlockSpec((2, rows, FF), lambda i: (0, i, 0)), weight, weight, tile, tile],
        [shape((TOK, D))], [tile], [], comms, number, 4 * TOK * D * FF, points,
    )


def place(at, k):
    return (at.x + (1 - 2 * at.x if k < 2 else 0)) * 2 + at.y + (1 - 2 * at.y if k in (1, 2) else 0)


def by_down(act, dy, comms, number):
    n = 4
    low, high = slice(0, 192), slice(192, 384)
    flows = ((1, 1), (1, 0), (0, 1), (0, 0))
    slots = ((1, 1), (0, None), (None, 0), (None, None))

    def body(at, step, ins, outs, scratch, landed):
        act_ref, dy_ref = ins
        kept, to_x, to_y = outs
        mine, send, recv, *sems = scratch

        def copy(t):
            return remote(send.at[t % 2], recv.at[t], sems[0:2], t, at.to_sib)

        @pl.when(step > 1)
        def _():
            copy(step - 2).wait_send()

        def product(core):
            half = act_ref[:, pl.ds(pl.multiple_of(core * 384, 128), 384)]
            return dot(half, dy_ref[...], 0, 0).astype(BF)

        send[step % 2] = product(1 - at.c)
        copy(step).start()
        mine[...] = product(at.c)

        for t in range(n):

            @pl.when(step == t)
            def _(t=t):
                copy(t).wait_recv()
                total = mine[...].astype(F32) + recv[t].astype(F32)
                a, b = total[low], total[high]
                if flows[t][0]:
                    to_x[slots[t][0]] = a.astype(BF)
                else:
                    kept[1 if flows[t][1] else 0, low, :] = a
                if flows[t][1]:
                    to_y[slots[t][1]] = b.astype(BF)
                else:
                    kept[1 if flows[t][0] else 0, high, :] = b

        @pl.when(step == n - 1)
        def _():
            copy(n - 2).wait_send()
            copy(n - 1).wait_send()

    def now(i):
        at = Place()
        fx, fy = 1 - i // 2, 1 - i % 2
        return 0, (at.x + fx * (1 - 2 * at.x)) * 2 + at.y + fy * (1 - 2 * at.y)

    whole = lambda *dims: pl.BlockSpec(dims, lambda i: (0,) * len(dims))
    return call(
        "by_down", body, (n,), [act, dy],
        [pl.BlockSpec((TOK, 768), now), once((TOK, D), lambda i: (0, 0))],
        [shape((2, 384, D), F32), shape((2, 192, D)), shape((2, 192, D))], [whole(2, 384, D), whole(2, 192, D), whole(2, 192, D)],
        [pltpu.VMEM((384, D), BF), pltpu.VMEM((2, 384, D), BF), pltpu.VMEM((n, 384, D), BF)] + [pltpu.SemaphoreType.DMA((n,)) for _ in range(2)],
        comms, number, 2 * TOK * D * FF,
    )


class Sum:
    def __init__(self, kept, far):
        self.kept, self.far = kept, far

    def next(self):
        return (self.kept[1] + self.far[1].astype(F32)).astype(BF)

    def cross(self):
        return Cross(self.next())

    def finish(self):
        return Finish(self.next(), self.kept, self.far)

    def rise(self, got):
        self.total = self.kept[0] + self.far[0].astype(F32) + got.astype(F32)
        return self.total.astype(BF)

    def end(self, got):
        return (self.total + got.astype(F32)).astype(BF)


def solution(mesh):
    def step(x, dy, w_gate, w_up, w_down):
        x, dy = x[0], dy[0]
        (a0, act0, gate0, up0), ((g0,), (u0,), (d0,)) = gate_up(x, w_gate, w_up, w_down, 0)
        early = [Gather(w_down, 1, 2), Gather(w_gate, 1, 4, (0,)), Gather(w_up, 1, 4, (0,))]
        when = {(0, 0, 1): 3, (0, 1, 1): 5, (0, 0, 2): 6, (1, 0, 0): 3, (2, 0, 0): 3, (1, 0, 1): 7, (2, 0, 1): 7, (0, 1, 2): 7}
        (h1, a1), ((d1,), (g1,), (u1,)) = down(act0, d0, x, early, 1, when)
        dgu1, s_gu1, (act1,), ((g1,), (u1,)) = middle(a1, dy, d1, None, ((w_gate, g1), (w_up, u1)), [], 2)
        (kept, *parts), _ = by_down(act1, dy, [], 3)
        (dh1,), ((got,), (far,)) = by_state(dgu1, g1, u1, h1, dy, [s_gu1.cross(), Spread(*parts)], 4)
        s_d1 = Sum(kept[:, None], far[:, None])
        (kept, *parts), ((got_d1,),) = by_down(act0, dh1, [s_d1.cross()], 5)
        comms = [Chain(kept, *parts), Rise(s_gu1.rise(got)), Rise(s_d1.rise(got_d1))]
        end_d0 = {(0, c, k): when for c in range(2) for k, when in ((1, 6), (2, 10), (3, 15))}
        dgu0, s_gu0, _, ((down0,), (z_gu1,), (z_d1,)) = middle(a0, dh1, d0, (gate0, up0), None, comms, 6, end_d0)
        end_gu0 = {(0, 0, 1): 1, (0, 1, 1): 2, (0, 2, 1): 3, (0, 3, 1): 4, (0, 0, 2): 4, (0, 1, 2): 6, (0, 2, 2): 7}
        (dx,), ((gu0,),) = by_state(dgu0, g0, u0, x, dh1, [s_gu0.finish()], 7, end_gu0)

        gu1, down1 = s_gu1.end(z_gu1), s_d1.end(z_d1)
        return dx[None], jnp.stack([gu0[0], gu1[0]]), jnp.stack([gu0[1], gu1[1]]), jnp.stack([down0, down1[0]])

    states, cut = P(("rep", "r", "s"), None, None), P(None, "s", None)
    return jax.shard_map(
        step,
        mesh=mesh,
        in_specs=(states, states) + (cut,) * 3,
        out_specs=(states,) + (P("rep", "s", None),) * 3,
        check_vma=False,
    )
```

```python
import functools

import jax
import jax.numpy as jnp
from jax import lax
from jax.experimental import pallas as pl
from jax.experimental.pallas import tpu as pltpu
from jax.sharding import PartitionSpec as P

MESH = pl.DeviceIdType.MESH
END = (1 << 30, 99)
BF, F32 = jnp.bfloat16, jnp.float32
ANY = pl.BlockSpec(memory_space=pl.ANY)
VMEM_LIMIT = 66_000_000
TOK, D, FF = 2048, 1280, 3072


class Place:
    def __init__(self):
        self.z = lax.axis_index("r")
        self.s = lax.axis_index("s")
        self.x = self.s // 4
        self.y = (self.s // 2) % 2
        self.c = self.s % 2
        self.xs = self.s + 4 - 8 * self.x
        self.ys = self.s + 2 - 4 * self.y
        self.sib = self.s + 1 - 2 * self.c
        self.ds = self.xs + 2 - 4 * self.y
        self.to_x, self.to_y, self.to_sib = {"s": self.xs}, {"s": self.ys}, {"s": self.sib}
        self.to_z = {"r": 1 - self.z}

    def greet(self):
        barrier = pltpu.get_barrier_semaphore()
        for peer in (self.to_x, self.to_y, self.to_sib, self.to_z):
            pl.semaphore_signal(barrier, inc=1, device_id=peer, device_id_type=MESH)
        pl.semaphore_wait(barrier, 4)


def remote(src, dst, sems, k, peer):
    return pltpu.make_async_remote_copy(
        src_ref=src, dst_ref=dst, send_sem=sems[0].at[k], recv_sem=sems[1].at[k], device_id=peer, device_id_type=MESH
    )


class Gather:
    copies = 14
    last = 4

    def __init__(self, whole, layer, blocks=1):
        self.inputs, self.layer, self.blocks = [whole], layer, blocks
        dims = whole.shape[1:]
        self.outputs = [jax.ShapeDtypeStruct((8, *dims), whole.dtype)]
        self.scratch = [
            pltpu.VMEM(dims, whole.dtype),
            pltpu.SemaphoreType.DMA((2,)),
            pltpu.SemaphoreType.DMA((self.copies * blocks,)),
            pltpu.SemaphoreType.DMA((self.copies * blocks,)),
        ]

    def stage(self, at, number, ins, outs, scratch, c=0):
        (whole,), (full,), (held, local, *sems) = ins, outs, scratch
        own = whole.at[self.layer]
        rows = own.shape[0]
        width = own.shape[1] // self.blocks
        cols = pl.ds(c * width, width)
        low = 48 if rows == 160 else rows // 3
        both = rows - low
        everything = pl.ds(0, rows)
        plane = pl.ds(pl.multiple_of(at.z * low, 16), both)
        middle = pl.ds(low, both - low)
        mine = pl.ds(pl.multiple_of(at.z * both, 16), low)
        theirs = pl.ds(pl.multiple_of((1 - at.z) * both, 16), low)

        def copy(k):
            def again(s, r, peer):
                return full.at[s, r, cols], full.at[s, r, cols], peer

            src, dst, peer = {
                0: lambda: (own.at[plane, cols], full.at[at.s, plane, cols], at.to_x),
                1: lambda: (own.at[plane, cols], full.at[at.s, plane, cols], at.to_y),
                2: lambda: (own.at[everything, cols], full.at[at.s, everything, cols], at.to_sib),
                3: lambda: again(at.xs, middle, at.to_y),
                4: lambda: again(at.ys, mine, at.to_x),
                5: lambda: again(at.xs, mine, at.to_z),
                6: lambda: again(at.ys, mine, at.to_z),
                7: lambda: again(at.xs, plane, at.to_sib),
                8: lambda: again(at.ys, plane, at.to_sib),
                9: lambda: again(at.ds, mine, at.to_z),
                10: lambda: again(at.ds, plane, at.to_sib),
                11: lambda: again(at.xs, theirs, at.to_sib),
                12: lambda: again(at.ys, theirs, at.to_sib),
                13: lambda: again(at.ds, theirs, at.to_sib),
            }[k]()
            return remote(src, dst, sems, self.copies * c + k, peer)

        into = lambda: pltpu.make_async_copy(own, held, local.at[0])
        out = lambda: pltpu.make_async_copy(held, full.at[at.s], local.at[1])
        wait, start = {
            0: ((), (0, 1, 2)),
            1: ((0, 1), (3, 4, 5, 6, 7, 8)),
            2: ((3, 4), (9, 10)),
            3: ((5, 6, 9), (11, 12, 13)),
            4: ((2, 7, 8, 10, 11, 12, 13), ()),
        }[number]
        if number == 1 and c == 0:
            into().wait()
            out().start()
        for k in wait:
            copy(k).wait_recv()
        for k in start:
            copy(k).start()
        if number == 0 and c == 0:
            into().start()
        if number == 4:
            for k in range(self.copies):
                copy(k).wait_send()
            if c == 0:
                out().wait()


class Cross:
    blocks, last = 1, 1

    def __init__(self, part):
        self.inputs = [part]
        self.outputs = [jax.ShapeDtypeStruct(part.shape, BF)]
        self.scratch = [pltpu.SemaphoreType.DMA((2,)), pltpu.SemaphoreType.DMA((2,))]

    def pairs(self, at, ins, outs):
        (part,), (got,) = ins, outs
        half = part.shape[1] // 2
        low, high = pl.ds(0, half), pl.ds(half, half)
        return [(part.at[:, low, :], got.at[:, low, :], at.to_y), (part.at[:, high, :], got.at[:, high, :], at.to_x)]

    def stage(self, at, number, ins, outs, scratch, c=0):
        for k, (src, dst, peer) in enumerate(self.pairs(at, ins, outs)):
            copy = remote(src, dst, scratch, k, peer)
            if number == 0:
                copy.start()
            else:
                copy.wait()


class Rise(Cross):
    def pairs(self, at, ins, outs):
        (part,), (got,) = ins, outs
        return [(part, got, at.to_z)]


class Finish:
    last = 3

    def __init__(self, part, kept, far):
        mats, rows, columns = part.shape
        self.inputs = [part, kept, far]
        self.outputs = [jax.ShapeDtypeStruct(part.shape, BF)]
        self.blocks, self.cut = 2 * mats, columns // 2
        each = (self.blocks, rows, self.cut)
        n = self.blocks
        self.scratch = [pltpu.VMEM(each, F32)] + [pltpu.VMEM(each, BF)] * 4
        self.scratch += [pltpu.SemaphoreType.DMA((n, 3)), pltpu.SemaphoreType.DMA((n, 3)), pltpu.SemaphoreType.DMA((n, 3))]

    def stage(self, at, number, ins, outs, scratch, c=0):
        (part, kept, far), (result,), (total, first, second, sent, third, *sems, local) = ins, outs, scratch
        rows = part.shape[1]
        half = rows // 2
        m, cols = c // 2, pl.ds(c % 2 * self.cut, self.cut)
        low, high = pl.ds(0, half), pl.ds(half, half)

        def along(k):
            r, peer = ((low, at.to_y), (high, at.to_x))[k]
            return pltpu.make_async_remote_copy(
                src_ref=part.at[m, r, cols], dst_ref=second.at[c, r, :], send_sem=sems[0].at[c, k], recv_sem=sems[1].at[c, k],
                device_id=peer, device_id_type=MESH,
            )

        def up():
            return pltpu.make_async_remote_copy(
                src_ref=sent.at[c], dst_ref=third.at[c], send_sem=sems[0].at[c, 2], recv_sem=sems[1].at[c, 2],
                device_id=at.to_z, device_id_type=MESH,
            )

        def loads():
            return [
                pltpu.make_async_copy(kept.at[0, m, :, cols], total.at[c], local.at[c, 0]),
                pltpu.make_async_copy(far.at[0, m, :, cols], first.at[c], local.at[c, 1]),
            ]

        def store():
            return pltpu.make_async_copy(sent.at[c], result.at[m, :, cols], local.at[c, 2])

        def each(f):
            @pl.loop(0, rows // 16)
            def _(k):
                f(pl.ds(pl.multiple_of(k * 16, 16), 16))

        if number == 0:
            for copy in (along(0), along(1), *loads()):
                copy.start()
        elif number == 1:
            for copy in (along(0), along(1), *loads()):
                copy.wait()

            def f(r):
                new = total[c, r, :] + first[c, r, :].astype(F32) + second[c, r, :].astype(F32)
                total[c, r, :] = new
                sent[c, r, :] = new.astype(BF)

            each(f)
            up().start()
        elif number == 2:
            up().wait()

            def f(r):
                sent[c, r, :] = (total[c, r, :] + third[c, r, :].astype(F32)).astype(BF)

            each(f)
            store().start()
        else:
            store().wait()


def call(name, body, grid, ins, in_specs, outs, out_specs, scratch, comms, number, flops, points=None):
    n_in, n_out, n_scratch = len(ins), len(outs), len(scratch)
    steps = functools.reduce(lambda a, b: a * b, grid, 1)
    points = points or {}
    events = {}
    for index, m in enumerate(comms):
        for c in range(m.blocks):
            for stage in range(m.last + 1):
                when = points.get((index, c, stage), 0 if stage == 0 else steps)
                when = when if isinstance(when, tuple) else (when, 0)
                events.setdefault(when if when[0] < steps else END, []).append((stage == 0, c, stage, index))

    def kernel(*refs):
        refs = list(refs)
        take = lambda n: [refs.pop(0) for _ in range(n)]
        i_refs = take(n_in)
        ci = [take(len(m.inputs)) for m in comms]
        o_refs = take(n_out)
        co = [take(len(m.outputs)) for m in comms]
        s_refs = take(n_scratch)
        cs = [take(len(m.scratch)) for m in comms]
        at = Place()
        step = pl.program_id(0)
        if len(grid) == 2:
            step = step * grid[1] + pl.program_id(1)

        @pl.when(step == 0)
        def _():
            at.greet()

        def happen(sub):
            for when, listed in events.items():
                if when[1] == sub:
                    order = sorted(listed, key=lambda e: (e[2], e[1], e[3])) if when == END else sorted(listed)

                    @pl.when(step == (steps - 1 if when == END else when[0]))
                    def _(order=order):
                        for _, c, stage, index in order:
                            comms[index].stage(at, stage, ci[index], co[index], cs[index], c)

        happen(0)
        body(at, step, i_refs, o_refs, s_refs, (co, happen))
        happen(END[1])

    flat = lambda key: [v for m in comms for v in getattr(m, key)]
    moved = flat("inputs")
    results = pl.pallas_call(
        kernel,
        grid=grid,
        in_specs=list(in_specs) + [ANY] * len(moved),
        out_specs=list(out_specs) + [ANY] * len(flat("outputs")),
        out_shape=list(outs) + flat("outputs"),
        scratch_shapes=list(scratch) + flat("scratch"),
        compiler_params=pltpu.CompilerParams(
            collective_id=number,
            has_side_effects=True,
            vmem_limit_bytes=VMEM_LIMIT,
            dimension_semantics=("arbitrary",) * len(grid),
        ),
        cost_estimate=pl.CostEstimate(flops=flops, bytes_accessed=1 << 24, transcendentals=0),
        name=name,
    )(*ins, *moved)
    results = list(results)
    mine, results = results[:n_out], results[n_out:]
    got = []
    for m in comms:
        got.append(results[: len(m.outputs)])
        results = results[len(m.outputs) :]
    return mine, got


def scale_of(wide):
    return lax.rsqrt(jnp.mean(wide * wide, -1, keepdims=True) + 1e-6)


def shape(dims, dtype=BF):
    return jax.ShapeDtypeStruct(dims, dtype)


def once(dims, index):
    return pl.BlockSpec(dims, index, pipeline_mode=pl.Buffered(1))


def dot(a, b, ca=1, cb=0):
    return lax.dot_general(a, b, (((ca,), (cb,)), ((), ())), preferred_element_type=F32)


def load_block(landed, buffers, sems, c, width):
    cols = pl.ds(c * width if isinstance(c, int) else pl.multiple_of(c * width, width), width)
    return [pltpu.make_async_copy(landed[m][0].at[:, :, cols], buffers.at[c % 2, m], sems.at[c % 2, m]) for m in range(2)]


def gate_up(x, w_gate, w_up, w_down, number):
    cols, blocks, lag = 512, FF // 512, 5

    def body(at, step, ins, outs, scratch, landed):
        x_ref = ins[0]
        a_out, act, gate, up = outs
        held, sems = scratch

        @pl.when(step == 0)
        def _():
            for k in range(TOK // 512):
                part = pl.ds(k * 512, 512)
                wide = x_ref[part, :].astype(F32)
                a_out[part, :] = (wide * scale_of(wide)).astype(BF)

        def load(c):
            for copy in load_block(arrived, held, sems, c, cols):
                copy.start()

        arrived, happen = landed

        @pl.when(step == lag - 1)
        def _():
            load(0)

        c = jnp.maximum(step - lag, 0)

        @pl.when(step >= lag)
        def _():
            for copy in load_block(arrived, held, sems, c, cols):
                copy.wait()

        for k in range(4):
            if k:
                happen(k)
            if k == 3:

                @pl.when((step >= lag) & (step < lag + blocks - 1))
                def _():
                    load(c + 1)

            @pl.when(step >= lag)
            def _(k=k):
                part = pl.ds(k * 512, 512)
                left = a_out[part, :]
                g = dot(left, held[c % 2, 0].reshape(D, cols))
                u = dot(left, held[c % 2, 1].reshape(D, cols))
                gate[part, :] = g
                up[part, :] = u
                act[part, :] = (g * jax.nn.sigmoid(g) * u).astype(BF)

    tile = pl.BlockSpec((TOK, cols), lambda i: (0, jnp.maximum(i - lag, 0)))
    whole = once((TOK, D), lambda i: (0, 0))
    comms = [Gather(w_gate, 0, blocks), Gather(w_up, 0, blocks), Gather(w_down, 0, 2)]
    when = {(0, k): k for k in range(5)} | {(1, 0): 1, (1, 1): lag - 1, (2, 0): lag - 1}
    for c in range(1, blocks + 1):
        rest = {(c + 1, 0): (lag + c - 2, 2), (c, 1): (lag + c - 2, 2), (c, 2): lag + c - 1, (c, 3): (lag + c - 1, 2), (c, 4): (lag + c - 1, 3)}
        when = rest | when
    points = {(m, c, k): when[c, k] for m in range(2) for c in range(blocks) for k in range(5)}
    points |= {(2, c, k): when[blocks - 1 + c, k] for c in range(2) for k in range(4)}
    return call(
        "gate_up", body, (blocks + lag,), [x], [whole], [shape((TOK, D)), shape((TOK, FF)), shape((TOK, FF), F32), shape((TOK, FF), F32)],
        [whole, tile, tile, tile], [pltpu.VMEM((2, 2, 8, 160, cols), BF), pltpu.SemaphoreType.DMA((2, 2))], comms, number, 4 * TOK * D * FF, points,
    )


def down(act, wd, h, comms, number, points):
    rows = 256

    def body(at, step, ins, outs, scratch, landed):
        act_ref, w_ref, h_ref = ins
        out = dot(act_ref[...], w_ref[...].reshape(FF, D)).astype(BF)
        new = (h_ref[...].astype(F32) + out.astype(F32)).astype(BF)
        outs[0][...] = new
        wide = new.astype(F32)
        outs[1][...] = (wide * scale_of(wide)).astype(BF)

    tile = pl.BlockSpec((rows, D), lambda i: (i, 0))
    return call(
        "down", body, (TOK // rows,), [act, wd, h], [pl.BlockSpec((rows, FF), lambda i: (i, 0)), once((8, 384, D), lambda i: (0, 0, 0)), tile],
        [shape((TOK, D)), shape((TOK, D))], [tile, tile], [], comms, number, 2 * TOK * D * FF, points,
    )


def middle(a, dy, wd, saved, weights, comms, number, extra=None):
    cols, rows = 768, 512
    blocks, tiles, n = FF // cols, TOK // rows, 2 * (FF // cols)
    lead = 5 if weights else 0
    steps = lead + blocks * tiles + 1
    across = TOK // tiles

    def body(at, step, ins, outs, scratch, landed):
        a_ref, dy_ref, wd_ref, *ins = ins
        d_out, kept, far, *outs = outs
        d_all, term, mine, send, recv, to_x, to_y, *sems = scratch
        t = step - lead
        j, i = t // tiles, t % tiles
        arrived, happen = landed

        def copy(u):
            return remote(send.at[u % 2], recv.at[u % 4], [s for s in sems[0:2]], u, at.to_sib)

        def there(u, half):
            return far.at[:, u % 2, pl.ds(80 * half, 80), pl.ds(pl.multiple_of(u // 2 * cols, cols), cols)]

        def along_x(u):
            return remote(to_x.at[u % 2], there(u, 0), sems[2:4], u, at.to_x)

        def along_y(u):
            return remote(to_y.at[u % 2], there(u, 1), sems[4:6], u, at.to_y)

        def finish(u):
            @pl.when(u > 1)
            def _():
                along_x(u - 2).wait_send()
                along_y(u - 2).wait_send()

            copy(u).wait_recv()
            slot = u % 2
            total = [mine[slot, k].astype(F32) + recv[u % 4, k].astype(F32) for k in range(4)]
            to_x[slot, 0] = total[0][:80].astype(BF)
            to_x[slot, 1] = total[1][:80].astype(BF)
            to_y[slot, 0] = total[2][80:].astype(BF)
            to_y[slot, 1] = total[1][80:].astype(BF)
            kept[0, 0] = total[3]
            kept[1, 0, :80] = total[2][:80]
            kept[1, 0, 80:] = total[0][80:]
            along_x(u).start()
            along_y(u).start()

        if weights:
            held, loads = scratch[-2:]

            @pl.when(step == lead - 1)
            def _():
                for load in load_block(arrived, held, loads, 0, cols):
                    load.start()

            @pl.when((t >= 0) & (t < blocks * tiles) & (i == 0))
            def _():
                for load in load_block(arrived, held, loads, j, cols):
                    load.wait()

        @pl.when((t >= 0) & (t < blocks * tiles))
        def _():
            sub = 256 if weights else 512
            w = wd_ref[...].reshape(cols, D)
            for k in range(rows // sub):
                here = pl.ds(k * sub, sub)
                if weights:
                    left = a_ref[pl.ds(pl.multiple_of(i * rows + k * sub, sub), sub), :]
                    g = dot(left, held[j % 2, 0].reshape(D, cols))
                    u = dot(left, held[j % 2, 1].reshape(D, cols))
                else:
                    g, u = ins[0][here, :], ins[1][here, :]
                da = dot(dy_ref[pl.ds(pl.multiple_of(i * rows + k * sub, sub), sub), :], w, 1, 1).astype(BF).astype(F32)
                sig = jax.nn.sigmoid(g)
                silu = g * sig
                if weights:
                    outs[0][here, :] = (silu * u).astype(BF)
                d_gate = (da * u * (sig + silu * (1 - sig))).astype(BF)
                d_up = (da * silu).astype(BF)
                d_out[0, here, :] = d_gate
                d_out[1, here, :] = d_up
                to = pl.ds(pl.multiple_of(i * rows + k * sub, sub), sub)
                d_all[0, to, :] = d_gate
                d_all[1, to, :] = d_up

        @pl.when((t > 0) & (i == 0))
        def _():
            finish(2 * j - 1)

        happen(1)
        if weights:

            @pl.when((t >= 0) & (t < (blocks - 1) * tiles) & (i == tiles - 1))
            def _():
                for load in load_block(arrived, held, loads, j + 1, cols):
                    load.start()

        @pl.when((t >= 0) & (t < blocks * tiles) & (i == tiles - 1))
        def _():
            for m in range(2):
                u = 2 * j + m

                @pl.when(u > 1)
                def _():
                    copy(u - 2).wait_send()

                term[...] = dot(a_ref[...], d_all[m], 0, 0).astype(BF).reshape(8, 160, cols)
                for k in range(4):
                    send[m, k] = term[2 * place(at, k) + 1 - at.c]
                    mine[m, k] = term[2 * place(at, k) + at.c]
                copy(u).start()
            finish(2 * j)

        @pl.when(step == steps - 1)
        def _():
            for u in (n - 2, n - 1):
                copy(u).wait_send()
                along_x(u).wait_send()
                along_y(u).wait_send()

            @pl.loop(0, n)
            def _(u):
                along_x(u).wait_recv()
                along_y(u).wait_recv()

    def block(s):
        t = jnp.clip(s - lead, 0, blocks * tiles - 1)
        return t // tiles, t % tiles

    def done(s):
        t = jnp.maximum(s - lead, 0)
        late = t % tiles == tiles - 1
        early = t < tiles - 1
        return 0, jnp.where(late | early, 0, 1), 0, jnp.where(late, t // tiles, jnp.maximum(t // tiles - 1, 0))

    tile = pl.BlockSpec((rows, cols), lambda s: (block(s)[1], block(s)[0]))
    sems = lambda: pltpu.SemaphoreType.DMA((n,))
    ins = [a, dy, wd] + (list(saved) if saved else [])
    in_specs = [once((TOK, D), lambda s: (0, 0)), once((TOK, D), lambda s: (0, 0)), pl.BlockSpec((2, 384, D), lambda s: (block(s)[0], 0, 0))]
    in_specs += [tile, tile] if saved else []
    scratch = [
        pltpu.VMEM((2, TOK, cols), BF), pltpu.VMEM((8, 160, cols), BF), pltpu.VMEM((2, 4, 160, cols), BF), pltpu.VMEM((2, 4, 160, cols), BF),
        pltpu.VMEM((4, 4, 160, cols), BF), pltpu.VMEM((2, 2, 80, cols), BF), pltpu.VMEM((2, 2, 80, cols), BF),
    ] + [sems() for _ in range(6)]
    points = extra
    if weights:
        comms = [Gather(weights[0], 1, blocks), Gather(weights[1], 1, blocks)] + comms
        scratch += [pltpu.VMEM((2, 2, 8, 160, cols), BF), pltpu.SemaphoreType.DMA((2, 2))]
        when = ((0, 1, 2, 3, 4), (1, 5, 7, 8, (8, 1)), (5, (8, 1), 9, 10, (12, 1)), ((8, 1), 9, 10, 11, (16, 1)))
        points = {(m, c, k): when[c][k] for m in range(2) for c in range(blocks) for k in range(5)}
    outs = [shape((2, TOK, FF)), shape((2, 2, 160, FF), F32), shape((2, 2, 160, FF))] + ([shape((TOK, FF))] if weights else [])
    out_specs = [
        pl.BlockSpec((2, rows, cols), lambda s: (0, block(s)[1], block(s)[0])), pl.BlockSpec((2, 1, 160, cols), done), ANY,
    ] + ([tile] if weights else [])
    (dgu, kept, far, *act), got = call(
        "middle", body, (steps,), ins, in_specs, outs, out_specs, scratch, comms, number, (10 if weights else 6) * TOK * D * FF, points,
    )
    return dgu, Sum(kept, far), act, got


def by_state(dgu, wg, wu, h, dy, comms, number, points=None):
    rows = 256

    def body(at, step, ins, outs, scratch, landed):
        d_ref, g_ref, u_ref, h_ref, dy_ref = ins
        first = dot(d_ref[0], g_ref[...].reshape(D, FF), 1, 1).astype(BF)
        second = dot(d_ref[1], u_ref[...].reshape(D, FF), 1, 1).astype(BF)
        da = (first.astype(F32) + second.astype(F32)).astype(BF).astype(F32)
        wide = h_ref[...].astype(F32)
        scale = scale_of(wide)
        along = jnp.sum(da * wide, -1, keepdims=True)
        dh = da * scale - wide * (along * scale * scale * scale * (1.0 / D))
        outs[0][...] = (dy_ref[...].astype(F32) + dh.astype(BF).astype(F32)).astype(BF)

    tile = pl.BlockSpec((rows, D), lambda i: (i, 0))
    weight = once((8, 160, FF), lambda i: (0, 0, 0))
    return call(
        "by_state", body, (TOK // rows,), [dgu, wg, wu, h, dy],
        [pl.BlockSpec((2, rows, FF), lambda i: (0, i, 0)), weight, weight, tile, tile],
        [shape((TOK, D))], [tile], [], comms, number, 4 * TOK * D * FF, points,
    )


def place(at, k):
    return (at.x + (1 - 2 * at.x if k < 2 else 0)) * 2 + at.y + (1 - 2 * at.y if k in (1, 2) else 0)


def by_down(act, dy, comms, number):
    n = 4
    low, high = slice(0, 192), slice(192, 384)
    flows = ((1, 1), (1, 0), (0, 1), (0, 0))
    slots = ((1, 1), (0, None), (None, 0), (None, None))

    def body(at, step, ins, outs, scratch, landed):
        act_ref, dy_ref = ins
        kept, far = outs
        mine, send, recv, to_x, to_y, *sems = scratch

        def copy(t):
            return remote(send.at[t % 2], recv.at[t], sems[0:2], t, at.to_sib)

        def along_x(t):
            return remote(to_x.at[t], far.at[slots[t][0], pl.ds(0, 192), :], sems[2:4], t, at.to_x)

        def along_y(t):
            return remote(to_y.at[t // 2], far.at[slots[t][1], pl.ds(192, 192), :], sems[4:6], t, at.to_y)

        @pl.when(step > 1)
        def _():
            copy(step - 2).wait_send()

        def product(core):
            half = act_ref[:, pl.ds(pl.multiple_of(core * 384, 128), 384)]
            return dot(half, dy_ref[...], 0, 0).astype(BF)

        send[step % 2] = product(1 - at.c)
        copy(step).start()
        mine[...] = product(at.c)

        for t in range(n):

            @pl.when(step == t)
            def _(t=t):
                copy(t).wait_recv()
                total = mine[...].astype(F32) + recv[t].astype(F32)
                a, b = total[low], total[high]
                if flows[t][0]:
                    to_x[t] = a.astype(BF)
                    along_x(t).start()
                else:
                    kept[1 if flows[t][1] else 0, low, :] = a
                if flows[t][1]:
                    to_y[t // 2] = b.astype(BF)
                    along_y(t).start()
                else:
                    kept[1 if flows[t][0] else 0, high, :] = b

        @pl.when(step == n - 1)
        def _():
            copy(n - 2).wait_send()
            copy(n - 1).wait_send()
            for t in range(n):
                if flows[t][0]:
                    along_x(t).wait()
                if flows[t][1]:
                    along_y(t).wait()

    def now(i):
        at = Place()
        fx, fy = 1 - i // 2, 1 - i % 2
        return 0, (at.x + fx * (1 - 2 * at.x)) * 2 + at.y + fy * (1 - 2 * at.y)

    sems = lambda: pltpu.SemaphoreType.DMA((n,))
    (kept, far), got = call(
        "by_down", body, (n,), [act, dy],
        [pl.BlockSpec((TOK, 768), now), once((TOK, D), lambda i: (0, 0))],
        [shape((2, 384, D), F32), shape((2, 384, D))], [pl.BlockSpec((2, 384, D), lambda i: (0, 0, 0)), ANY],
        [pltpu.VMEM((384, D), BF), pltpu.VMEM((2, 384, D), BF), pltpu.VMEM((n, 384, D), BF),
         pltpu.VMEM((2, 192, D), BF), pltpu.VMEM((2, 192, D), BF)] + [sems() for _ in range(6)],
        comms, number, 2 * TOK * D * FF,
    )
    return Sum(kept[:, None], far[:, None]), got


class Sum:
    def __init__(self, kept, far):
        self.kept, self.far = kept, far

    def next(self):
        return (self.kept[1] + self.far[1].astype(F32)).astype(BF)

    def cross(self):
        return Cross(self.next())

    def finish(self):
        return Finish(self.next(), self.kept, self.far)

    def rise(self, got):
        self.total = self.kept[0] + self.far[0].astype(F32) + got.astype(F32)
        return self.total.astype(BF)

    def end(self, got):
        return (self.total + got.astype(F32)).astype(BF)


def solution(mesh):
    def step(x, dy, w_gate, w_up, w_down):
        x, dy = x[0], dy[0]
        (a0, act0, gate0, up0), ((g0,), (u0,), (d0,)) = gate_up(x, w_gate, w_up, w_down, 0)
        (h1, a1), ((d1,),) = down(act0, d0, x, [Gather(w_down, 1, 2)], 1, {(0, 0, 1): 3, (0, 1, 1): 6, (0, 0, 2): 7})
        dgu1, s_gu1, (act1,), ((g1,), (u1,)) = middle(a1, dy, d1, None, (w_gate, w_up), [], 2)
        s_d1, _ = by_down(act1, dy, [], 3)
        (dh1,), ((got,), (got_d1,)) = by_state(dgu1, g1, u1, h1, dy, [s_gu1.cross(), s_d1.cross()], 4)
        s_d0, ((z_d1,),) = by_down(act0, dh1, [Rise(s_d1.rise(got_d1))], 5)
        end_d0 = {(0, 0, 1): 3, (0, 1, 1): 4, (0, 0, 2): 14, (0, 1, 2): 15}
        dgu0, s_gu0, _, ((down0,), (z_gu1,)) = middle(a0, dh1, d0, (gate0, up0), None, [s_d0.finish(), Rise(s_gu1.rise(got))], 6, end_d0)
        end_gu0 = {(0, 0, 1): 1, (0, 1, 1): 2, (0, 2, 1): 3, (0, 3, 1): 4, (0, 0, 2): 4, (0, 1, 2): 6, (0, 2, 2): 7}
        (dx,), ((gu0,),) = by_state(dgu0, g0, u0, x, dh1, [s_gu0.finish()], 7, end_gu0)

        gu1, down1 = s_gu1.end(z_gu1), s_d1.end(z_d1)
        return dx[None], jnp.stack([gu0[0], gu1[0]]), jnp.stack([gu0[1], gu1[1]]), jnp.stack([down0[0], down1[0]])

    states, cut = P(("rep", "r", "s"), None, None), P(None, "s", None)
    return jax.shard_map(
        step,
        mesh=mesh,
        in_specs=(states, states) + (cut,) * 3,
        out_specs=(states,) + (P("rep", "s", None),) * 3,
        check_vma=False,
    )
```
